32 devices in a mesh: branch: 2 (over core), dp: 4 (over y, x), mp: 4 (over z).
Axes of the slice: x: 2, y: 2, z: 4, core: 2. Of those that a mesh axis runs over, the one named last changes fastest.
Arguments:
- unet_hidden: bfloat16 [8, 1280, 256], P(('branch', 'dp'), 'mp'), may hold values from -6 to 6
- control_hidden: bfloat16 [2, 2, 4, 1280, 256], P('branch', None, 'dp', 'mp'), may hold values from -6 to 6
- timesteps: int32 [2, 4], P(None, 'dp'), may hold values from 0 to 999
- control_scales: int32 [2, 2, 4], P('branch', None, 'dp'), may hold values from 1 to 16
- unet_time_first: bfloat16 [320, 1280], replicated, may hold values from -0.3125 to 0.3125
- unet_time_second: bfloat16 [1280, 1280], replicated, may hold values from -0.15625 to 0.15625
- unet_proj: bfloat16 [1280, 1280], P(None, 'mp'), may hold values from -0.15625 to 0.15625
- unet_conv_first: bfloat16 [9, 1280, 1280], P(None, 'mp'), may hold values from -0.0546875 to 0.0546875
- unet_conv_second: bfloat16 [9, 1280, 1280], P(None, 'mp'), may hold values from -0.0546875 to 0.0546875
- control_time_first: bfloat16 [2, 320, 1280], P('branch'), may hold values from -0.3125 to 0.3125
- control_time_second: bfloat16 [2, 1280, 1280], P('branch'), may hold values from -0.15625 to 0.15625
- control_proj: bfloat16 [2, 1280, 1280], P('branch', None, 'mp'), may hold values from -0.15625 to 0.15625
- control_conv_first: bfloat16 [2, 9, 1280, 1280], P('branch', None, 'mp'), may hold values from -0.0546875 to 0.0546875
- control_conv_second: bfloat16 [2, 9, 1280, 1280], P('branch', None, 'mp'), may hold values from -0.0546875 to 0.0546875
- zero_conv: bfloat16 [2, 1280, 1280], P('branch', 'mp'), may hold values from -0.15625 to 0.15625
Outputs:
- skip_out: bfloat16 [8, 1280, 256], P(('branch', 'dp'), 'mp')
The draws below stay inside these ranges and needn't reach their ends.
All inputs are finite; a program needn't handle non-finite values.
Results may differ from the reference program's by a relative error of at most 0.018.
Values may be sent and summed in bfloat16 or wider, within the bound.
A program may use at most 128 MiB of HBM per device.

```python
import math
import jax
import jax.numpy as jnp
from jax import lax

C = 1280
TDIM = 320
GROUPS = 32
SIDE = 16
COPIES = 2
HW = 256
HALVES = 2
BATCH = 8


def plant(entries, key, smallest, high):
    index_at = [jax.random.randint(jax.random.fold_in(key, axis), (), 0, length) for axis, length in enumerate(entries.shape)]
    main_axis = entries.shape.index(max(entries.shape))
    beside = index_at[:main_axis] + [(index_at[main_axis] + 1) % entries.shape[main_axis]] + index_at[main_axis + 1:]
    return entries.at[tuple(index_at)].set(smallest).at[tuple(beside)].set(high)


def shard_levels(rng, extent, split, smallest, top_value):
    factor_of, own = 1.0, jax.random.fold_in(rng, 6)
    for dim, parts in split:
        heights = jnp.exp(jax.random.uniform(jax.random.fold_in(own, dim), (parts,), jnp.float32, smallest / len(split), top_value / len(split)))
        factor_of = factor_of * jnp.repeat(heights, extent[dim] // parts).reshape([-1 if axis == dim else 1 for axis in range(len(extent))])
    return factor_of


def centred(stream_key, extent, deviation, most, cuts=(), held_as=jnp.bfloat16):
    level = shard_levels(stream_key, extent, cuts, -0.22, 0.18) if cuts else 1.0
    array = jax.random.normal(stream_key, extent, jnp.float32) * deviation * level
    return jnp.minimum(jnp.maximum(array, -most), most).astype(held_as)


def setup_inputs(seed: int = 0) -> dict:
    key_list = jax.random.split(jax.random.key(seed), 16)
    unet_hidden = centred(key_list[0], (BATCH, C, HW), 1.0, 6.0, ((0, 8), (1, 4)))
    control_hidden = centred(key_list[1], (COPIES, HALVES, BATCH // HALVES, C, HW), 1.0, 6.0, ((0, 2), (2, 4), (3, 4)))
    timesteps = plant(jax.random.randint(key_list[2], (HALVES, BATCH // HALVES), 0, 1000), jax.random.fold_in(key_list[2], 1), 0, 999).astype(jnp.int32)
    control_scales = plant(jax.random.randint(key_list[3], (COPIES, HALVES, BATCH // HALVES), 1, 17), jax.random.fold_in(key_list[3], 1), 1, 16).astype(jnp.int32)
    unet_time_first = centred(key_list[4], (TDIM, C), TDIM ** -0.5, 0.3125)
    unet_time_second = centred(key_list[5], (C, C), C ** -0.5, 0.15625)
    unet_proj = centred(key_list[6], (C, C), C ** -0.5, 0.15625, ((1, 4),))
    unet_conv_first = centred(key_list[7], (9, C, C), (9 * C) ** -0.5, 0.0546875, ((1, 4),))
    unet_conv_second = centred(key_list[8], (9, C, C), (9 * C) ** -0.5, 0.0546875, ((1, 4),))
    control_time_first = centred(key_list[9], (COPIES, TDIM, C), TDIM ** -0.5, 0.3125, ((0, 2),))
    control_time_second = centred(key_list[10], (COPIES, C, C), C ** -0.5, 0.15625, ((0, 2),))
    control_proj = centred(key_list[11], (COPIES, C, C), C ** -0.5, 0.15625, ((0, 2), (2, 4)))
    control_conv_first = centred(key_list[12], (COPIES, 9, C, C), (9 * C) ** -0.5, 0.0546875, ((0, 2), (2, 4)))
    control_conv_second = centred(key_list[13], (COPIES, 9, C, C), (9 * C) ** -0.5, 0.0546875, ((0, 2), (2, 4)))
    zero_conv = centred(key_list[14], (COPIES, C, C), C ** -0.5, 0.15625, ((0, 2), (1, 4)))
    return dict(unet_hidden=unet_hidden, control_hidden=control_hidden, timesteps=timesteps, control_scales=control_scales, unet_time_first=unet_time_first, unet_time_second=unet_time_second, unet_proj=unet_proj, unet_conv_first=unet_conv_first, unet_conv_second=unet_conv_second, control_time_first=control_time_first, control_time_second=control_time_second, control_proj=control_proj, control_conv_first=control_conv_first, control_conv_second=control_conv_second, zero_conv=zero_conv)


def sinusoid(step_ids):
    half_width = TDIM // 2
    frequency = jnp.exp(-math.log(10000.0) * jnp.arange(half_width, dtype=jnp.float32) / half_width)
    angles = step_ids.astype(jnp.float32)[:, None] * frequency[None, :]
    return jnp.concatenate([jnp.cos(angles), jnp.sin(angles)], axis=1)

def time_embed(step_ids, first_weight, second_weight):
    waves = sinusoid(step_ids).astype(jnp.bfloat16)
    middle = jax.nn.silu(jnp.dot(waves, first_weight, preferred_element_type=jnp.float32)).astype(jnp.bfloat16)
    embedded = jnp.dot(middle, second_weight, preferred_element_type=jnp.float32)
    return jax.nn.silu(embedded).astype(jnp.bfloat16)

def norm_silu(values):
    image_count, width, pixels = values.shape
    group_size = C // GROUPS
    grouped = values.reshape(image_count, width // group_size, group_size, pixels)
    group_mean = lax.optimization_barrier(jnp.mean(grouped, axis=(2, 3), keepdims=True))
    centered = grouped - group_mean
    group_var = lax.optimization_barrier(jnp.mean(centered * centered, axis=(2, 3), keepdims=True))
    normed = centered * lax.rsqrt(group_var + 1e-05)
    return jax.nn.silu(normed).reshape(image_count, width, pixels)

def conv_taps(activation, weight, einsum_form):
    image_count, width, pixels = activation.shape
    image_grid = activation.astype(jnp.float32).reshape(image_count, width, SIDE, SIDE)
    padded = jnp.pad(image_grid, ((0, 0), (0, 0), (1, 1), (1, 1)))
    accum_sum = None
    for tap_index in range(9):
        row_shift = tap_index // 3
        col_shift = tap_index % 3
        window = padded[:, :, row_shift:row_shift + SIDE, col_shift:col_shift + SIDE].reshape(image_count, width, pixels)
        term = jnp.einsum(einsum_form, weight[tap_index].astype(jnp.float32), window, precision=lax.Precision.HIGHEST)
        accum_sum = term if accum_sum is None else accum_sum + term
    return accum_sum

def resnet_block(hidden, conv_first, conv_second, time_proj, time_act):
    first_act = norm_silu(hidden.astype(jnp.float32)).astype(jnp.bfloat16)
    inner_sum = conv_taps(first_act, conv_first, 'oc,bcp->bop')
    inner_sum = inner_sum + jnp.dot(time_act, time_proj, preferred_element_type=jnp.float32)[:, :, None]
    second_act = norm_silu(inner_sum).astype(jnp.bfloat16)
    return hidden.astype(jnp.float32) + conv_taps(second_act, conv_second, 'co,bcp->bop')

def reference(unet_hidden, control_hidden, timesteps, control_scales, unet_time_first, unet_time_second, unet_proj, unet_conv_first, unet_conv_second, control_time_first, control_time_second, control_proj, control_conv_first, control_conv_second, zero_conv):
    step_ids = timesteps.reshape(BATCH)
    unet_act = time_embed(step_ids, unet_time_first, unet_time_second)
    unet_out = resnet_block(unet_hidden, unet_conv_first, unet_conv_second, unet_proj, unet_act)
    residual = jnp.zeros((BATCH, C, HW), jnp.float32)
    for copy_index in range(COPIES):
        copy_act = time_embed(step_ids, control_time_first[copy_index], control_time_second[copy_index])
        copy_hidden = control_hidden[copy_index].reshape(BATCH, C, HW)
        copy_out = resnet_block(copy_hidden, control_conv_first[copy_index], control_conv_second[copy_index], control_proj[copy_index], copy_act).astype(jnp.bfloat16)
        scale_factor = control_scales[copy_index].reshape(BATCH).astype(jnp.float32) / 8.0
        zero_terms = jnp.einsum('co,bcp->bop', zero_conv[copy_index].astype(jnp.float32), copy_out.astype(jnp.float32), precision=lax.Precision.HIGHEST)
        residual = residual + scale_factor[:, None, None] * zero_terms
    return (unet_out + residual).astype(jnp.bfloat16)
```

```python
import functools
import math

import jax
import jax.numpy as jnp
from jax import lax
from jax.experimental import pallas as pl
from jax.experimental.pallas import tpu as pltpu
from jax.sharding import PartitionSpec as P

TDIM = 320
GROUP = 40
PIECES = 2
SIDE = 16
MESH = pl.DeviceIdType.MESH


def sinusoid(steps, rows):
    half_width = TDIM // 2
    row = lax.broadcasted_iota(jnp.int32, (rows, TDIM), 0)
    spot = lax.broadcasted_iota(jnp.int32, (rows, TDIM), 1)
    place = jnp.where(spot < half_width, spot, spot - half_width).astype(jnp.float32)
    frequency = jnp.exp(-math.log(10000.0) * place / half_width)
    step = jnp.zeros((rows, TDIM), jnp.float32)
    for i, value in enumerate(steps):
        step = jnp.where(row == i, value.astype(jnp.float32), step)
    angles = step * frequency
    return jnp.where(spot < half_width, jnp.cos(angles), jnp.sin(angles))


def norm_silu(values):
    width, pixels = values.shape
    grouped = values.reshape(width // GROUP, GROUP, pixels)
    count = 1.0 / (GROUP * pixels)
    mean = jnp.sum(jnp.sum(grouped, axis=1, keepdims=True), axis=2, keepdims=True) * count
    centered = grouped - mean
    var = jnp.sum(jnp.sum(centered * centered, axis=1, keepdims=True), axis=2, keepdims=True) * count
    normed = centered * lax.rsqrt(var + 1e-05)
    return jax.nn.silu(normed).reshape(width, pixels)


def kernel(
    ways,
    unet_hidden,
    control_hidden,
    steps,
    scale,
    hbm_time_first_c,
    hbm_time_second_c,
    hbm_proj_c,
    hbm_time_first_u,
    hbm_time_second_u,
    hbm_proj_u,
    first_c,
    second_c,
    first_u,
    second_u,
    zero,
    out,
    time_first,
    time_second,
    proj,
    w1c,
    w2c,
    w1u,
    w2u,
    wz,
    gathered,
    above,
    below,
    taps,
    start,
    inner,
    sends,
    lands,
    scaled,
    swap_out,
    swap_in,
    load_sem,
    ag_send,
    ag_recv,
    rs_send,
    rs_recv,
    swap_send,
    swap_recv,
):
    branch = lax.axis_index("branch")
    dp = lax.axis_index("dp")
    me = lax.axis_index("mp")
    width, pixels = unet_hidden.shape[1], unet_hidden.shape[2]
    channels = ways * width
    last = ways - 1
    half = pixels // PIECES
    scope = jax.named_scope

    loads = [
        pltpu.make_async_copy(src, dst, load_sem.at[i])
        for i, (src, dst) in enumerate(
            (
                (hbm_time_first_c, time_first.at[0]),
                (hbm_time_second_c, time_second.at[0]),
                (hbm_proj_c, proj.at[0]),
                (hbm_time_first_u, time_first.at[1]),
                (hbm_time_second_u, time_second.at[1]),
                (hbm_proj_u, proj.at[1]),
                (first_c, w1c),
                (second_c, w2c),
                (first_u, w1u),
                (second_u, w2u),
                (zero, wz),
            )
        )
    ]
    for i in (0, 1, 2, 6):
        loads[i].start()

    barrier = pltpu.get_barrier_semaphore()

    def greet(inside, coord):
        @pl.when(inside)
        def _():
            pl.semaphore_signal(barrier, inc=1, device_id=coord, device_id_type=MESH)

    greet(me < last, (branch, dp, me + 1))
    greet(me > 0, (branch, dp, me - 1))
    pl.semaphore_signal(barrier, inc=1, device_id=(1 - branch, dp, me), device_id_type=MESH)

    def wait_barrier():
        edge = (me == 0) | (me == last)

        @pl.when(edge)
        def _():
            pl.semaphore_wait(barrier, 2)

        @pl.when(jnp.logical_not(edge))
        def _():
            pl.semaphore_wait(barrier, 3)

    def part(piece):
        return pl.ds(piece * half, half)

    def rows_of(slot):
        return pl.ds(pl.multiple_of(slot * width, width), width)

    def ag_copy(unit, side, hop, slot, piece):
        return pltpu.make_async_remote_copy(
            src_ref=gathered.at[unit, rows_of(slot), part(piece)],
            dst_ref=gathered.at[unit, rows_of(slot), part(piece)],
            send_sem=ag_send.at[unit, side, hop, piece],
            recv_sem=ag_recv.at[unit, side, hop, piece],
            device_id=(branch, dp, me + 1 - 2 * side),
            device_id_type=MESH,
        )

    middle = ways // 2

    def forward(unit, hop, sides):
        for piece in range(PIECES):
            for side in range(2):
                from_slot = me - hop if side == 0 else me + hop
                here = (from_slot >= 0) & (from_slot <= last)
                onward = here & ((me < last) if side == 0 else (me > 0)) & sides[side]

                @pl.when(onward)
                def _():
                    if hop > 0:
                        ag_copy(unit, side, hop - 1, from_slot, piece).wait_recv()
                    ag_copy(unit, side, hop, from_slot, piece).start()

    low, high = me < middle, me >= middle
    edge = (me == 0) | (me == last)
    inner_low, inner_high = low & jnp.logical_not(edge), high & jnp.logical_not(edge)
    both, inward, outward = (True, True), (low, high), (high, low)

    def ag_begin(unit, sides=both):
        forward(unit, 0, sides)

    def ag_inward(unit):
        for hop in range(1, last):
            forward(unit, hop, inward)

    def ag_outward(unit, hop):
        forward(unit, hop, outward)

    def ag_arrive(unit):
        for hop in range(1, ways):
            for side in range(2):
                from_slot = me - hop if side == 0 else me + hop
                here = (from_slot >= 0) & (from_slot <= last)
                if hop < last:
                    here = here & ((me == last) if side == 0 else (me == 0))

                @pl.when(here)
                def _():
                    for piece in range(PIECES):
                        ag_copy(unit, side, hop - 1, from_slot, piece).wait_recv()

    def ag_drain(unit):
        for hop in range(last):
            for side in range(2):
                from_slot = me - hop if side == 0 else me + hop
                here = (from_slot >= 0) & (from_slot <= last)
                onward = here & ((me < last) if side == 0 else (me > 0))

                @pl.when(onward)
                def _():
                    for piece in range(PIECES):
                        ag_copy(unit, side, hop, from_slot, piece).wait_send()

    def rs_copy(unit, side, dest, piece):
        return pltpu.make_async_remote_copy(
            src_ref=sends.at[unit, rows_of(dest), part(piece)],
            dst_ref=lands.at[unit, side, dest, :, part(piece)],
            send_sem=rs_send.at[unit, dest, piece],
            recv_sem=rs_recv.at[unit, side, dest, piece],
            device_id=(branch, dp, me + 1 - 2 * side),
            device_id_type=MESH,
        )

    def rs_start(unit):
        @pl.when(me == 0)
        def _():
            for dest in range(last, 0, -1):
                for piece in range(PIECES):
                    rs_copy(unit, 0, dest, piece).start()

        @pl.when(me == last)
        def _():
            for dest in range(last):
                for piece in range(PIECES):
                    rs_copy(unit, 1, dest, piece).start()

    def rs_slot(unit, slot):
        for piece, side in [(p, d) for p in range(PIECES) for d in range(2)]:
            place = me if side == 0 else last - me
            dest = last - slot + place if side == 0 else slot - place

            @pl.when((place >= 1) & (place <= slot))
            def _():
                rs_copy(unit, side, dest, piece).wait_recv()
                added = sends[unit, rows_of(dest), part(piece)].astype(jnp.float32) + lands[
                    unit, side, dest, :, part(piece)
                ].astype(jnp.float32)
                sends[unit, rows_of(dest), part(piece)] = added.astype(jnp.bfloat16)
                rs_copy(unit, side, dest, piece).start()

    def rs_drain(unit):
        for dest in range(ways):

            @pl.when(dest > me)
            def _():
                for piece in range(PIECES):
                    rs_copy(unit, 0, dest, piece).wait_send()

            @pl.when(dest < me)
            def _():
                for piece in range(PIECES):
                    rs_copy(unit, 1, dest, piece).wait_send()

    def own_hidden(unit):
        if unit == 2:
            return unet_hidden[0]
        image = 1 - branch if unit == 0 else branch
        return control_hidden[0, image, 0]

    def prepare(unit):
        gathered[unit, rows_of(me), :] = norm_silu(own_hidden(unit).astype(jnp.float32)).astype(
            jnp.bfloat16
        )

    def embed(block, waves):
        for load in loads[3 * block : 3 * block + 3]:
            load.wait()
        act = waves
        for weight in (time_first, time_second):
            act = jax.nn.silu(
                jnp.dot(act, weight[block], preferred_element_type=jnp.float32)
            ).astype(jnp.bfloat16)
        start[block] = lax.dot_general(
            proj[block], act, (((1,), (1,)), ((), ())), preferred_element_type=jnp.float32
        )

    def column_kept(shape, axis, dx):
        spot = lax.rem(lax.broadcasted_iota(jnp.int32, shape, axis), SIDE) + dx
        return (spot >= 0) & (spot < SIDE)

    def shift_rows(unit):
        spot = lax.broadcasted_iota(jnp.int32, (1, pixels), 1)
        whole = gathered[unit].astype(jnp.float32)
        down = pltpu.roll(whole, SIDE, 1)
        above[...] = jnp.where(spot >= SIDE, down, 0.0).astype(jnp.bfloat16)
        up = pltpu.roll(whole, pixels - SIDE, 1)
        below[...] = jnp.where(spot < pixels - SIDE, up, 0.0).astype(jnp.bfloat16)

    def first_conv(unit, weight, hook):
        shift_rows(unit)
        other = branch == 1 if unit == 0 else branch == 0
        columns = start[unit // 2]
        bias = jnp.where(other, columns[:, :1], columns[:, 1:2])

        def side_term(dx):
            term = None
            for line, source in enumerate((above[...], gathered[unit], below[...])):
                product = jnp.dot(
                    weight[3 * line + dx + 1], source, preferred_element_type=jnp.float32
                )
                term = product if term is None else term + product
            return term

        inner[...] = side_term(0) + bias
        hook(0)
        for dx in (-1, 1):
            moved = pltpu.roll(side_term(dx), (pixels - dx) % pixels, 1)
            inner[...] += jnp.where(column_kept((1, pixels), 1, dx), moved, 0.0)
            hook(dx)

    def fill_taps():
        flipped = norm_silu(inner[...]).T
        operands = []
        for dx in (-1, 0, 1):
            moved = flipped if dx == 0 else pltpu.roll(flipped, (pixels - dx) % pixels, 0)
            operands.append(jnp.where(column_kept((pixels, 1), 0, dx), moved, 0.0))
        taps[SIDE : SIDE + pixels, :] = jnp.concatenate(operands, axis=1).astype(jnp.bfloat16)

    def second_conv(unit, weight, hook):
        tile = channels // 5
        for chunk in range(5):
            at = pl.ds(chunk * tile, tile)
            total = None
            for line in range(3):
                product = jnp.dot(
                    taps[SIDE * line : SIDE * line + pixels, :],
                    weight[3 * line : 3 * line + 3, :, chunk * tile : (chunk + 1) * tile].reshape(
                        3 * width, tile
                    ),
                    preferred_element_type=jnp.float32,
                )
                total = product if total is None else total + product
            if unit == 2:
                total = total + jnp.dot(
                    scaled[...],
                    wz[:, chunk * tile : (chunk + 1) * tile],
                    preferred_element_type=jnp.float32,
                )
                total = total + swap_in[:, chunk * tile : (chunk + 1) * tile].astype(jnp.float32)
            sends[unit, at, :] = total.T.astype(jnp.bfloat16)
            hook(chunk)

    def collect(unit):
        result = own_hidden(unit).astype(jnp.float32) + sends[unit, rows_of(me), :].astype(
            jnp.float32
        )
        inner[...] = result
        for side, inside in ((0, me > 0), (1, me < last)):

            @pl.when(inside)
            def _():
                for piece in range(PIECES):
                    rs_copy(unit, side, me, piece).wait_recv()
                inner[...] += lands[unit, side, me].astype(jnp.float32)

        return inner[...]

    def scale_copy(unit):
        image = 1 - branch if unit == 0 else branch
        factor = scale[0, image].astype(jnp.float32) * 0.125
        scaled[...] = (collect(unit) * factor).T.astype(jnp.bfloat16)

    def quiet(place):
        pass

    taps[0:SIDE, :] = jnp.zeros((SIDE, 3 * width), jnp.bfloat16)
    taps[SIDE + pixels :, :] = jnp.zeros((SIDE, 3 * width), jnp.bfloat16)

    hops = range(1, last)
    with scope("prep"):
        for unit in range(3):
            prepare(unit)
        waves = sinusoid([steps[0, i] for i in range(steps.shape[1])], 16).astype(jnp.bfloat16)
    with scope("barrier"):
        wait_barrier()
    with scope("ag0"):
        ag_begin(0)
        for unit in (1, 2):
            ag_begin(unit, (me == 0, me == last))
    with scope("embed0"):
        embed(0, waves)
        for i in (7, 3, 4, 5):
            loads[i].start()
    for hop in hops:
        with scope(f"ag0_hop{hop}"):
            forward(0, hop, both)
            if hop == 1:
                ag_begin(1, (inner_low, inner_high))
    with scope("ag1"):
        ag_begin(1, outward)
        ag_inward(1)
    with scope("ag0_wait"):
        ag_arrive(0)
    with scope("w1c_wait"):
        loads[6].wait()
    with scope("conv1_0"):
        first_conv(0, w1c, quiet)
    with scope("ag2_in"):
        ag_begin(2, (inner_low, inner_high))
        ag_inward(2)
    with scope("ag1_out1"):
        ag_outward(1, 1)
    with scope("w2c_wait"):
        loads[7].wait()
    with scope("fill0"):
        fill_taps()
    with scope("conv2_0"):
        second_conv(0, w2c, quiet)
    for hop in hops[1:]:
        with scope(f"ag1_out{hop}"):
            ag_outward(1, hop)
    with scope("ag2"):
        ag_begin(2, outward)
    with scope("rs0"):
        rs_start(0)
        for i in (8, 9, 10):
            loads[i].start()
    with scope("embed1"):
        embed(1, waves)
    with scope("rs0_slot1"):
        rs_slot(0, 1)
    with scope("ag1_wait"):
        ag_arrive(1)
    with scope("conv1_1"):
        first_conv(1, w1c, quiet)
    with scope("ag2_out1"):
        ag_outward(2, 1)
    with scope("rs0_slot2"):
        for slot in hops[1:]:
            rs_slot(0, slot)
    with scope("fill1"):
        fill_taps()
    with scope("conv2_1"):
        second_conv(1, w2c, quiet)
    for hop in hops[1:]:
        with scope(f"ag2_out{hop}"):
            ag_outward(2, hop)
    with scope("rs1"):
        rs_start(1)
    with scope("res0"):
        loads[10].wait()
        scale_copy(0)
        swap_out[...] = jnp.dot(scaled[...], wz[...], preferred_element_type=jnp.float32).astype(
            jnp.bfloat16
        )
    swap = pltpu.make_async_remote_copy(
        src_ref=swap_out,
        dst_ref=swap_in,
        send_sem=swap_send,
        recv_sem=swap_recv,
        device_id=(1 - branch, dp, me),
        device_id_type=MESH,
    )
    swap.start()
    with scope("rs1_slot1"):
        rs_slot(1, 1)
    with scope("ag2_wait"):
        ag_arrive(2)
        loads[8].wait()
        loads[9].wait()
    with scope("conv1_2"):
        first_conv(2, w1u, quiet)
    with scope("rs1_slot2"):
        for slot in hops[1:]:
            rs_slot(1, slot)
    with scope("fill2"):
        fill_taps()
    with scope("res1"):
        scale_copy(1)
    with scope("swap_wait"):
        swap.wait_recv()
    with scope("conv2_2"):
        second_conv(2, w2u, quiet)
    with scope("rs2"):
        rs_start(2)
    for slot in hops:
        with scope(f"rs2_slot{slot}"):
            rs_slot(2, slot)
    with scope("collect2"):
        out[0] = collect(2).astype(jnp.bfloat16)
    swap.wait_send()
    for unit in range(3):
        ag_drain(unit)
        rs_drain(unit)

def shards(
    unet_hidden,
    control_hidden,
    timesteps,
    control_scales,
    unet_time_first,
    unet_time_second,
    unet_proj,
    unet_conv_first,
    unet_conv_second,
    control_time_first,
    control_time_second,
    control_proj,
    control_conv_first,
    control_conv_second,
    zero_conv,
):
    ways = lax.axis_size("mp")
    width, pixels = unet_hidden.shape[1], unet_hidden.shape[2]
    channels = ways * width
    halves = timesteps.shape[0]
    steps = timesteps.reshape(1, halves)
    scale = control_scales.reshape(1, halves)
    vmem = pl.BlockSpec(memory_space=pltpu.VMEM)
    smem = pl.BlockSpec(memory_space=pltpu.SMEM)
    hbm = pl.BlockSpec(memory_space=pl.ANY)
    taps = unet_conv_first.shape[0]
    bf16, f32 = jnp.bfloat16, jnp.float32
    conv_shape = (taps, width, channels)
    return pl.pallas_call(
        functools.partial(kernel, ways),
        out_shape=jax.ShapeDtypeStruct((1, width, pixels), bf16),
        in_specs=[vmem] * 2 + [smem] * 2 + [hbm] * 11,
        out_specs=vmem,
        scratch_shapes=[
            pltpu.VMEM((2,) + unet_time_first.shape, bf16),
            pltpu.VMEM((2,) + unet_time_second.shape, bf16),
            pltpu.VMEM((2,) + unet_proj.shape[::-1], bf16),
            pltpu.VMEM(conv_shape, bf16),
            pltpu.VMEM(conv_shape, bf16),
            pltpu.VMEM(conv_shape, bf16),
            pltpu.VMEM(conv_shape, bf16),
            pltpu.VMEM((width, channels), bf16),
            pltpu.VMEM((3, channels, pixels), bf16),
            pltpu.VMEM((channels, pixels), bf16),
            pltpu.VMEM((channels, pixels), bf16),
            pltpu.VMEM((pixels + 2 * SIDE, 3 * width), bf16),
            pltpu.VMEM((2, width, 16), f32),
            pltpu.VMEM((width, pixels), f32),
            pltpu.VMEM((3, channels, pixels), bf16),
            pltpu.VMEM((3, 2, ways, width, pixels), bf16),
            pltpu.VMEM((pixels, width), bf16),
            pltpu.VMEM((pixels, channels), bf16),
            pltpu.VMEM((pixels, channels), bf16),
            pltpu.SemaphoreType.DMA((11,)),
            pltpu.SemaphoreType.DMA((3, 2, ways - 1, PIECES)),
            pltpu.SemaphoreType.DMA((3, 2, ways - 1, PIECES)),
            pltpu.SemaphoreType.DMA((3, ways, PIECES)),
            pltpu.SemaphoreType.DMA((3, 2, ways, PIECES)),
            pltpu.SemaphoreType.DMA,
            pltpu.SemaphoreType.DMA,
        ],
        compiler_params=pltpu.CompilerParams(
            collective_id=0, has_side_effects=True, vmem_limit_bytes=62 * 1024 * 1024
        ),
    )(
        unet_hidden,
        control_hidden,
        steps,
        scale,
        control_time_first[0],
        control_time_second[0],
        control_proj[0].T,
        unet_time_first,
        unet_time_second,
        unet_proj.T,
        control_conv_first[0],
        control_conv_second[0],
        unet_conv_first,
        unet_conv_second,
        zero_conv[0],
    )


def solution(mesh):
    in_specs = (
        P(("branch", "dp"), "mp", None),
        P("branch", None, "dp", "mp", None),
        P(None, "dp"),
        P("branch", None, "dp"),
        P(),
        P(),
        P(None, "mp"),
        P(None, "mp", None),
        P(None, "mp", None),
        P("branch", None, None),
        P("branch", None, None),
        P("branch", None, "mp"),
        P("branch", None, "mp", None),
        P("branch", None, "mp", None),
        P("branch", "mp", None),
    )
    out_specs = P(("branch", "dp"), "mp", None)
    return jax.shard_map(shards, mesh=mesh, in_specs=in_specs, out_specs=out_specs, check_vma=False)
```

```python
import functools
import math

import jax
import jax.numpy as jnp
from jax import lax
from jax.experimental import pallas as pl
from jax.experimental.pallas import tpu as pltpu
from jax.sharding import PartitionSpec as P

TDIM = 320
GROUP = 40
PIECES = 2
PAIR_PIECES = 4
EDGE_FIRST = 2
SIDE = 16
MESH = pl.DeviceIdType.MESH


def sinusoid(steps, rows):
    half_width = TDIM // 2
    row = lax.broadcasted_iota(jnp.int32, (rows, TDIM), 0)
    spot = lax.broadcasted_iota(jnp.int32, (rows, TDIM), 1)
    place = jnp.where(spot < half_width, spot, spot - half_width).astype(jnp.float32)
    frequency = jnp.exp(-math.log(10000.0) * place / half_width)
    step = jnp.zeros((rows, TDIM), jnp.float32)
    for i, value in enumerate(steps):
        step = jnp.where(row == i, value.astype(jnp.float32), step)
    angles = step * frequency
    return jnp.where(spot < half_width, jnp.cos(angles), jnp.sin(angles))


def norm_silu(values):
    width, pixels = values.shape
    grouped = values.reshape(width // GROUP, GROUP, pixels)
    count = 1.0 / (GROUP * pixels)
    mean = jnp.sum(jnp.sum(grouped, axis=1, keepdims=True), axis=2, keepdims=True) * count
    centered = grouped - mean
    var = jnp.sum(jnp.sum(centered * centered, axis=1, keepdims=True), axis=2, keepdims=True) * count
    normed = centered * lax.rsqrt(var + 1e-05)
    return jax.nn.silu(normed).reshape(width, pixels)


def kernel(
    ways,
    unet_hidden,
    control_hidden,
    steps,
    scale,
    hbm_time_first_c,
    hbm_time_second_c,
    hbm_proj_c,
    hbm_time_first_u,
    hbm_time_second_u,
    hbm_proj_u,
    first_c,
    second_c,
    first_u,
    second_u,
    zero,
    out,
    time_first,
    time_second,
    proj,
    w1c,
    w2c,
    w1u,
    w2u,
    wz,
    gathered,
    above,
    below,
    taps,
    start,
    inner,
    sends,
    lands,
    far,
    pair_lands,
    pair_total,
    held,
    scaled,
    swap_out,
    swap_in,
    load_sem,
    ag_send,
    ag_recv,
    rs_send,
    rs_recv,
    far_recv,
    pair_send,
    pair_recv,
    z_send,
    z_recv,
    swap_send,
    swap_recv,
):
    branch = lax.axis_index("branch")
    dp = lax.axis_index("dp")
    me = lax.axis_index("mp")
    width, pixels = unet_hidden.shape[1], unet_hidden.shape[2]
    channels = ways * width
    last = ways - 1
    tile = 256
    chunks = channels // tile
    scope = jax.named_scope

    loads = [
        pltpu.make_async_copy(src, dst, load_sem.at[i])
        for i, (src, dst) in enumerate(
            (
                (hbm_time_first_c, time_first.at[0]),
                (hbm_time_second_c, time_second.at[0]),
                (hbm_proj_c, proj.at[0]),
                (hbm_time_first_u, time_first.at[1]),
                (hbm_time_second_u, time_second.at[1]),
                (hbm_proj_u, proj.at[1]),
                (first_c, w1c),
                (second_c, w2c),
                (first_u, w1u),
                (second_u, w2u),
                (zero, wz.at[pl.ds(pl.multiple_of(lax.rem(me, 2) * width, width), width)]),
            )
        )
    ]
    for i in (0, 1, 2, 6):
        loads[i].start()

    barrier = pltpu.get_barrier_semaphore()

    def greet(inside, coord):
        @pl.when(inside)
        def _():
            pl.semaphore_signal(barrier, inc=1, device_id=coord, device_id_type=MESH)

    greet(me < last, (branch, dp, me + 1))
    greet(me > 0, (branch, dp, me - 1))
    pl.semaphore_signal(barrier, inc=1, device_id=(1 - branch, dp, me), device_id_type=MESH)

    planes = lax.axis_size("dp")
    for place in range(planes):

        @pl.when(dp != place)
        def _():
            pl.semaphore_signal(barrier, inc=1, device_id=(branch, place, me), device_id_type=MESH)

    def wait_barrier():
        rim = (me == 0) | (me == last)

        @pl.when(rim)
        def _():
            pl.semaphore_wait(barrier, 1 + planes)

        @pl.when(jnp.logical_not(rim))
        def _():
            pl.semaphore_wait(barrier, 2 + planes)

    def rows_of(slot, piece=None):
        if piece is None:
            return pl.ds(pl.multiple_of(slot * width, width), width)
        size = width // PIECES
        return pl.ds(pl.multiple_of(slot * width + piece * size, size), size)

    def strip(piece):
        return pl.ds(piece * (width // PIECES), width // PIECES)

    middle = ways // 2
    low, high = me < middle, me >= middle

    def ag_copy(unit, side, hop, slot, piece):
        return pltpu.make_async_remote_copy(
            src_ref=gathered.at[unit, rows_of(slot, piece)],
            dst_ref=gathered.at[unit, rows_of(slot, piece)],
            send_sem=ag_send.at[unit, side, hop, piece],
            recv_sem=ag_recv.at[unit, side, hop, piece],
            device_id=(branch, dp, me + 1 - 2 * side),
            device_id_type=MESH,
        )


    def forward(unit, hop, sides):
        for piece in range(PIECES):
            for side, half in ((0, low), (1, high), (0, high), (1, low)):
                if half is (high if side == 0 else low) and sides is inward:
                    continue
                if half is (low if side == 0 else high) and sides is outward:
                    continue
                from_slot = me - hop if side == 0 else me + hop
                here = (from_slot >= 0) & (from_slot <= last)
                onward = here & ((me < last) if side == 0 else (me > 0)) & half & sides[side]

                @pl.when(onward)
                def _():
                    if hop > 0:
                        ag_copy(unit, side, hop - 1, from_slot, piece).wait_recv()
                    ag_copy(unit, side, hop, from_slot, piece).start()

    low, high = me < middle, me >= middle

    def ag_copy(unit, side, hop, slot, piece):
        return pltpu.make_async_remote_copy(
            src_ref=gathered.at[unit, rows_of(slot, piece)],
            dst_ref=gathered.at[unit, rows_of(slot, piece)],
            send_sem=ag_send.at[unit, side, hop, piece],
            recv_sem=ag_recv.at[unit, side, hop, piece],
            device_id=(branch, dp, me + 1 - 2 * side),
            device_id_type=MESH,
        )


    def forward(unit, hop, sides):
        for piece in range(PIECES):
            for side in range(2):
                from_slot = me - hop if side == 0 else me + hop
                here = (from_slot >= 0) & (from_slot <= last)
                onward = here & ((me < last) if side == 0 else (me > 0)) & sides[side]

                @pl.when(onward)
                def _():
                    if hop > 0:
                        ag_copy(unit, side, hop - 1, from_slot, piece).wait_recv()
                    ag_copy(unit, side, hop, from_slot, piece).start()

    edge = (me == 0) | (me == last)
    centre = jnp.logical_not(edge)
    inner_low, inner_high = low & jnp.logical_not(edge), high & jnp.logical_not(edge)
    both, inward, outward = (True, True), (low, high), (high, low)

    def ag_begin(unit, sides=both):
        forward(unit, 0, sides)

    def ag_inward(unit):
        for hop in range(1, last):
            forward(unit, hop, inward)

    def ag_outward(unit, hop):
        forward(unit, hop, outward)

    def ag_arrive(unit, passed):
        for hop in passed:
            for side in range(2):
                from_slot = me - hop if side == 0 else me + hop
                here = (from_slot >= 0) & (from_slot <= last)
                if hop < last:
                    here = here & ((me == last) if side == 0 else (me == 0))

                @pl.when(here)
                def _():
                    for piece in range(PIECES):
                        ag_copy(unit, side, hop - 1, from_slot, piece).wait_recv()

    def ag_drain(unit):
        for hop in range(last):
            for side in range(2):
                from_slot = me - hop if side == 0 else me + hop
                here = (from_slot >= 0) & (from_slot <= last)
                onward = here & ((me < last) if side == 0 else (me > 0))

                @pl.when(onward)
                def _():
                    for piece in range(PIECES):
                        ag_copy(unit, side, hop, from_slot, piece).wait_send()

    def rs_copy(side, dest, piece):
        return pltpu.make_async_remote_copy(
            src_ref=sends.at[2, rows_of(dest, piece)],
            dst_ref=lands.at[side, dest, strip(piece)],
            send_sem=rs_send.at[dest, piece],
            recv_sem=rs_recv.at[side, dest, piece],
            device_id=(branch, dp, me + 1 - 2 * side),
            device_id_type=MESH,
        )

    def far_copy(dest, piece):
        return pltpu.make_async_remote_copy(
            src_ref=sends.at[2, rows_of(dest, piece)],
            dst_ref=far.at[strip(piece)],
            send_sem=rs_send.at[dest, piece],
            recv_sem=far_recv.at[piece],
            device_id=(branch, dp, dest),
            device_id_type=MESH,
        )

    def fold_begin(group):
        ready = EDGE_FIRST * tile // width
        for rank in range(ready) if group == 0 else range(ready, last):
            for side, end in ((0, 0), (1, last)):
                dest = last - rank if side == 0 else rank

                @pl.when(me == end)
                def _():
                    for piece in range(PIECES):
                        rs_copy(side, dest, piece).start()

        if group == 0:
            return
        for side in range(2):
            rim = middle - side
            for dest in range(rim + 1, ways) if side == 0 else range(rim):

                @pl.when((me == rim) & centre)
                def _():
                    for piece in range(PIECES):
                        rs_copy(side, dest, piece).start()

    def fold_slots():
        for rank, piece, side in [
            (r, p, d) for r in range(last - 1) for p in range(PIECES) for d in range(2)
        ]:
            dest = last - rank if side == 0 else rank
            place = me if side == 0 else last - me
            rim = (place == middle - 1) & (rank < middle)
            onward = (place >= 1) & (place != middle) & (place < last - rank)

            @pl.when(onward)
            def _():
                rs_copy(side, dest, piece).wait_recv()
                added = sends[2, rows_of(dest, piece), :].astype(jnp.float32) + lands[
                    side, dest, strip(piece), :
                ].astype(jnp.float32)
                sends[2, rows_of(dest, piece), :] = added.astype(jnp.bfloat16)

            @pl.when(onward & rim)
            def _():
                far_copy(dest, piece).start()

            @pl.when(onward & jnp.logical_not(rim))
            def _():
                rs_copy(side, dest, piece).start()

    def fold_drain():
        for dest in range(ways):

            @pl.when(me != dest)
            def _():
                for piece in range(PIECES):
                    rs_copy(0, dest, piece).wait_send()

    double = 2 * width
    pairs = ways // 2
    mine = me // 2
    parity = lax.rem(me, 2)
    inwards = jnp.where(low, me + 1, me - 1)
    side_near = jnp.where(low, 0, 1)
    side_far = jnp.where(low, 1, 0)
    part = double // PAIR_PIECES

    def pair_copy(unit, side, pair, piece):
        return pltpu.make_async_remote_copy(
            src_ref=sends.at[unit, pl.ds(pair * double + piece * part, part)],
            dst_ref=pair_lands.at[unit, side, pair, pl.ds(piece * part, part)],
            send_sem=pair_send.at[unit, pair, piece],
            recv_sem=pair_recv.at[unit, side, pair, piece],
            device_id=(branch, dp, me + 1 - 2 * side),
            device_id_type=MESH,
        )

    def pair_order(side):
        return range(pairs - 1, -1, -1) if side == 0 else range(pairs)

    def pair_begin(unit):
        for side, end in ((0, 0), (1, last)):

            @pl.when(me == end)
            def _():
                for pair in pair_order(side):
                    if pair != end // 2:
                        for piece in range(PAIR_PIECES):
                            pair_copy(unit, side, pair, piece).start()

    def pair_slot(unit):
        for side in range(2):
            for pair in pair_order(side):
                beyond = (pair > mine) if side == 0 else (pair < mine)

                @pl.when(centre & beyond)
                def _():
                    for piece in range(PAIR_PIECES):
                        pair_copy(unit, side, pair, piece).wait_recv()
                        rows = pl.ds(pair * double + piece * part, part)
                        added = sends[unit, rows, :].astype(jnp.float32) + pair_lands[
                            unit, side, pair, pl.ds(piece * part, part), :
                        ].astype(jnp.float32)
                        sends[unit, rows, :] = added.astype(jnp.bfloat16)
                        pair_copy(unit, side, pair, piece).start()

    def pair_drain(unit):
        for pair in range(pairs):
            for side, beyond in ((0, pair > mine), (1, pair < mine)):

                @pl.when(beyond)
                def _():
                    for piece in range(PAIR_PIECES):
                        pair_copy(unit, side, pair, piece).wait_send()

    shares = math.gcd(width // 8, planes)
    share = width // shares
    sharing = dp < shares
    mate = me + 1 - 2 * parity

    def share_rows(holder, place):
        row = lax.rem(holder, 2) * width + place * share
        return pl.ds(pl.multiple_of(row, share), share)

    def cross_copy():
        return pltpu.make_async_remote_copy(
            src_ref=zero.at[pl.ds(pl.multiple_of(dp * share, share), share)],
            dst_ref=wz.at[share_rows(me, dp)],
            send_sem=z_send.at[dp],
            recv_sem=z_recv.at[dp],
            device_id=(branch, dp, mate),
            device_id_type=MESH,
        )

    def cross_begin(chosen):
        @pl.when(chosen & sharing)
        def _():
            cross_copy().start()

    def plane_copy(source, target):
        return pltpu.make_async_remote_copy(
            src_ref=wz.at[share_rows(mate, source)],
            dst_ref=wz.at[share_rows(mate, source)],
            send_sem=z_send.at[target],
            recv_sem=z_recv.at[source],
            device_id=(branch, target, me),
            device_id_type=MESH,
        )

    def plane_begin():
        @pl.when(sharing)
        def _():
            cross_copy().wait_recv()

        for place in range(planes):

            @pl.when(sharing & (dp != place))
            def _():
                plane_copy(dp, place).start()

    def plane_arrive():
        loads[10].wait()
        for place in range(shares):

            @pl.when(dp != place)
            def _():
                plane_copy(place, place).wait_recv()

    def plane_drain():
        @pl.when(sharing)
        def _():
            cross_copy().wait_send()

        for place in range(planes):

            @pl.when(sharing & (dp != place))
            def _():
                plane_copy(dp, place).wait_send()

    def own_hidden(unit):
        if unit == 2:
            return unet_hidden[0]
        image = 1 - branch if unit == 0 else branch
        return control_hidden[0, image, 0]

    def prepare(unit):
        gathered[unit, rows_of(me), :] = norm_silu(own_hidden(unit).astype(jnp.float32)).astype(
            jnp.bfloat16
        )

    def embed(block, waves):
        for load in loads[3 * block : 3 * block + 3]:
            load.wait()
        act = waves
        for weight in (time_first, time_second):
            act = jax.nn.silu(
                jnp.dot(act, weight[block], preferred_element_type=jnp.float32)
            ).astype(jnp.bfloat16)
        start[block] = lax.dot_general(
            proj[block], act, (((1,), (1,)), ((), ())), preferred_element_type=jnp.float32
        )

    def column_kept(shape, axis, dx):
        spot = lax.rem(lax.broadcasted_iota(jnp.int32, shape, axis), SIDE) + dx
        return (spot >= 0) & (spot < SIDE)

    def shift_rows(unit, rows):
        spot = lax.broadcasted_iota(jnp.int32, (1, pixels), 1)
        whole = gathered[unit, rows, :].astype(jnp.float32)
        down = pltpu.roll(whole, SIDE, 1)
        above[rows, :] = jnp.where(spot >= SIDE, down, 0.0).astype(jnp.bfloat16)
        up = pltpu.roll(whole, pixels - SIDE, 1)
        below[rows, :] = jnp.where(spot < pixels - SIDE, up, 0.0).astype(jnp.bfloat16)

    def first_conv(unit, weight, half=None):
        if half is None:
            rows = slice(0, channels)
        else:
            rows = pl.ds(pl.multiple_of(half * (channels // 2), channels // 2), channels // 2)
        shift_rows(unit, rows)

        def side_term(dx):
            term = None
            sources = (above[rows, :], gathered[unit, rows, :], below[rows, :])
            for line, source in enumerate(sources):
                product = jnp.dot(
                    weight[3 * line + dx + 1, :, rows],
                    source,
                    preferred_element_type=jnp.float32,
                )
                term = product if term is None else term + product
            return term

        if half is side_far:
            inner[...] += side_term(0)
        else:
            other = branch == 1 if unit == 0 else branch == 0
            columns = start[unit // 2]
            inner[...] = side_term(0) + jnp.where(other, columns[:, :1], columns[:, 1:2])
        for dx in (-1, 1):
            moved = pltpu.roll(side_term(dx), (pixels - dx) % pixels, 1)
            inner[...] += jnp.where(column_kept((1, pixels), 1, dx), moved, 0.0)

    def fill_taps():
        flipped = norm_silu(inner[...]).T
        operands = []
        for dx in (-1, 0, 1):
            moved = flipped if dx == 0 else pltpu.roll(flipped, (pixels - dx) % pixels, 0)
            operands.append(jnp.where(column_kept((pixels, 1), 0, dx), moved, 0.0))
        taps[SIDE : SIDE + pixels, :] = jnp.concatenate(operands, axis=1).astype(jnp.bfloat16)


    def columns_of(chunk):
        return slice(chunk * tile, (chunk + 1) * tile)

    def second_chunk(weight, chunk):
        total = None
        for line in range(3):
            product = jnp.dot(
                taps[SIDE * line : SIDE * line + pixels, :],
                weight[3 * line : 3 * line + 3, :, columns_of(chunk)].reshape(3 * width, tile),
                preferred_element_type=jnp.float32,
            )
            total = product if total is None else total + product
        return total

    def residual_chunk(chunk):
        at = columns_of(chunk)
        term = jnp.dot(scaled[...], wz[:, at], preferred_element_type=jnp.float32)
        return term + swap_in[:, at].astype(jnp.float32)

    def second_conv(unit, weight):
        for chunk in range(chunks):
            total = second_chunk(weight, chunk)
            sends[unit, columns_of(chunk), :] = total.T.astype(jnp.bfloat16)
        pair_begin(unit)

    def edge_conv(order, first):
        for chunk in order[:first]:
            total = second_chunk(w2u, chunk) + residual_chunk(chunk)
            sends[2, columns_of(chunk), :] = total.T.astype(jnp.bfloat16)

    def edge_last():
        for half, order in ((low, range(chunks - 1, -1, -1)), (high, range(chunks))):

            @pl.when(half)
            def _():
                edge_conv(order, EDGE_FIRST)
                if EDGE_FIRST < chunks:
                    fold_begin(0)
                    edge_conv(order[EDGE_FIRST:], chunks)

        if EDGE_FIRST == chunks:
            fold_begin(0)
        fold_begin(1)

    def centre_conv():
        for chunk in range(chunks):
            held[columns_of(chunk), :] = second_chunk(w2u, chunk).T

    def centre_last():
        for chunk in range(chunks):
            at = columns_of(chunk)
            sends[2, at, :] = (held[at, :] + residual_chunk(chunk).T).astype(jnp.bfloat16)
        fold_begin(1)

    def collect():
        inner[...] = own_hidden(2).astype(jnp.float32) + sends[2, rows_of(me), :].astype(
            jnp.float32
        )
        left, right = (me > 0) & (me != middle), (me < last) & (me != middle - 1)
        for side, inside in ((0, left), (1, right)):

            @pl.when(inside)
            def _():
                for piece in range(PIECES):
                    rs_copy(side, me, piece).wait_recv()
                inner[...] += lands[side, me].astype(jnp.float32)

        for piece in range(PIECES):
            far_copy(inwards, piece).wait_recv()
        return inner[...] + far[...].astype(jnp.float32)

    def scale_copy(unit):
        image = 1 - branch if unit == 0 else branch
        factor = scale[0, image].astype(jnp.float32) * 0.125
        pair_total[...] = sends[
            unit, pl.ds(pl.multiple_of(mine * double, double), double), :
        ].astype(jnp.float32)
        own = pl.ds(pl.multiple_of(parity * width, width), width)
        pair_total[own, :] += own_hidden(unit).astype(jnp.float32)
        for pair in range(pairs):
            for side in range(2):

                @pl.when(centre & (mine == pair) & (parity == side))
                def _():
                    for piece in range(PAIR_PIECES):
                        pair_copy(unit, side, pair, piece).wait_recv()
                    pair_total[...] += pair_lands[unit, side, pair].astype(jnp.float32)

        scaled[...] = (pair_total[...] * factor).T.astype(jnp.bfloat16)

    swap = pltpu.make_async_remote_copy(
        src_ref=swap_out,
        dst_ref=swap_in,
        send_sem=swap_send,
        recv_sem=swap_recv,
        device_id=(1 - branch, dp, me),
        device_id_type=MESH,
    )

    def first_residual():
        scale_copy(0)
        swap_out[...] = jnp.dot(scaled[...], wz[...], preferred_element_type=jnp.float32).astype(
            jnp.bfloat16
        )
        swap.start()

    taps[0:SIDE, :] = jnp.zeros((SIDE, 3 * width), jnp.bfloat16)
    taps[SIDE + pixels :, :] = jnp.zeros((SIDE, 3 * width), jnp.bfloat16)

    hops = range(1, last)
    with scope("prep"):
        for unit in range(3):
            prepare(unit)
        waves = sinusoid([steps[0, i] for i in range(steps.shape[1])], 16).astype(jnp.bfloat16)
    with scope("barrier"):
        wait_barrier()
    with scope("ag0"):
        ag_begin(0)
        cross_begin(centre)
        for unit in (1, 2):
            ag_begin(unit, (me == 0, me == last))
        cross_begin(edge)
    with scope("embed0"):
        embed(0, waves)
        for i in (7, 3, 4, 5, 10):
            loads[i].start()
    for hop in hops:
        with scope(f"ag0_hop{hop}"):
            forward(0, hop, both)
            if hop == 1:
                ag_begin(1, (inner_low, inner_high))
    with scope("ag1"):
        ag_begin(1, outward)
        ag_inward(1)
    with scope("embed1"):
        embed(1, waves)
    with scope("ag0_wait"):
        ag_arrive(0, range(1, ways))
    with scope("w1c_wait"):
        loads[6].wait()
    with scope("conv1_0"):
        first_conv(0, w1c)
    with scope("ag2_in"):
        ag_begin(2, (inner_low, inner_high))
        ag_inward(2)
    with scope("ag1_out1"):
        ag_outward(1, 1)
        for i in (8, 9):
            loads[i].start()
    with scope("w2c_wait"):
        loads[7].wait()
    with scope("fill0"):
        fill_taps()
    with scope("conv2_0"):
        second_conv(0, w2c)
    for hop in hops[1:]:
        with scope(f"ag1_out{hop}"):
            ag_outward(1, hop)
    with scope("ag2"):
        ag_begin(2, outward)
    with scope("plane"):
        plane_begin()
    with scope("ag1_wait"):
        ag_arrive(1, range(1, ways))
    with scope("conv1_1"):
        first_conv(1, w1c)
    with scope("ag2_out1"):
        ag_outward(2, 1)
    with scope("fill1"):
        fill_taps()
    for hop in hops[1:]:
        with scope(f"ag2_out{hop}"):
            ag_outward(2, hop)
    with scope("conv2_1"):
        second_conv(1, w2c)
    with scope("rs0_slot"):
        pair_slot(0)
    with scope("plane_wait"):
        plane_arrive()
    with scope("res0e"):
        pl.when(edge)(first_residual)
    with scope("ag2_wait"):
        ag_arrive(2, range(1, middle))
        loads[8].wait()
    with scope("conv1_2n"):
        first_conv(2, w1u, side_near)
    with scope("ag2_wait2"):
        ag_arrive(2, range(middle, ways))
        loads[9].wait()
    with scope("conv1_2f"):
        first_conv(2, w1u, side_far)
    with scope("res0c"):
        pl.when(centre)(first_residual)
    with scope("fill2"):
        fill_taps()

    @pl.when(edge)
    def _():
        with scope("res1e"):
            scale_copy(1)
        with scope("swap_e"):
            swap.wait_recv()
        with scope("conv2_2e"):
            edge_last()

    @pl.when(centre)
    def _():
        with scope("conv2_2c"):
            centre_conv()
        with scope("rs1_slot"):
            pair_slot(1)
        with scope("res1c"):
            scale_copy(1)
        with scope("swap_c"):
            swap.wait_recv()
        with scope("add_c"):
            centre_last()

    with scope("rs2_slots"):
        fold_slots()
    with scope("collect2"):
        out[0] = collect().astype(jnp.bfloat16)
    with scope("drain"):
        swap.wait_send()
        plane_drain()
        for unit in range(3):
            ag_drain(unit)
        for unit in range(2):
            pair_drain(unit)
        fold_drain()


def shards(
    unet_hidden,
    control_hidden,
    timesteps,
    control_scales,
    unet_time_first,
    unet_time_second,
    unet_proj,
    unet_conv_first,
    unet_conv_second,
    control_time_first,
    control_time_second,
    control_proj,
    control_conv_first,
    control_conv_second,
    zero_conv,
):
    ways, planes = lax.axis_size("mp"), lax.axis_size("dp")
    width, pixels = unet_hidden.shape[1], unet_hidden.shape[2]
    channels = ways * width
    halves = timesteps.shape[0]
    steps = timesteps.reshape(1, halves)
    scale = control_scales.reshape(1, halves)
    vmem = pl.BlockSpec(memory_space=pltpu.VMEM)
    smem = pl.BlockSpec(memory_space=pltpu.SMEM)
    hbm = pl.BlockSpec(memory_space=pl.ANY)
    taps = unet_conv_first.shape[0]
    bf16, f32 = jnp.bfloat16, jnp.float32
    conv_shape = (taps, width, channels)
    return pl.pallas_call(
        functools.partial(kernel, ways),
        out_shape=pltpu.VMEM((1, width, pixels), bf16),
        in_specs=[vmem] * 2 + [smem] * 2 + [hbm] * 11,
        out_specs=vmem,
        scratch_shapes=[
            pltpu.VMEM((2,) + unet_time_first.shape, bf16),
            pltpu.VMEM((2,) + unet_time_second.shape, bf16),
            pltpu.VMEM((2,) + unet_proj.shape[::-1], bf16),
            pltpu.VMEM(conv_shape, bf16),
            pltpu.VMEM(conv_shape, bf16),
            pltpu.VMEM(conv_shape, bf16),
            pltpu.VMEM(conv_shape, bf16),
            pltpu.VMEM((2 * width, channels), bf16),
            pltpu.VMEM((3, channels, pixels), bf16),
            pltpu.VMEM((channels, pixels), bf16),
            pltpu.VMEM((channels, pixels), bf16),
            pltpu.VMEM((pixels + 2 * SIDE, 3 * width), bf16),
            pltpu.VMEM((2, width, 16), f32),
            pltpu.VMEM((width, pixels), f32),
            pltpu.VMEM((3, channels, pixels), bf16),
            pltpu.VMEM((2, ways, width, pixels), bf16),
            pltpu.VMEM((width, pixels), bf16),
            pltpu.VMEM((2, 2, ways // 2, 2 * width, pixels), bf16),
            pltpu.VMEM((2 * width, pixels), f32),
            pltpu.VMEM((channels, pixels), f32),
            pltpu.VMEM((pixels, 2 * width), bf16),
            pltpu.VMEM((pixels, channels), bf16),
            pltpu.VMEM((pixels, channels), bf16),
            pltpu.SemaphoreType.DMA((11,)),
            pltpu.SemaphoreType.DMA((3, 2, ways - 1, PIECES)),
            pltpu.SemaphoreType.DMA((3, 2, ways - 1, PIECES)),
            pltpu.SemaphoreType.DMA((ways, PIECES)),
            pltpu.SemaphoreType.DMA((2, ways, PIECES)),
            pltpu.SemaphoreType.DMA((PIECES,)),
            pltpu.SemaphoreType.DMA((2, ways // 2, PAIR_PIECES)),
            pltpu.SemaphoreType.DMA((2, 2, ways // 2, PAIR_PIECES)),
            pltpu.SemaphoreType.DMA((planes,)),
            pltpu.SemaphoreType.DMA((planes,)),
            pltpu.SemaphoreType.DMA,
            pltpu.SemaphoreType.DMA,
        ],
        compiler_params=pltpu.CompilerParams(
            collective_id=0, has_side_effects=True, vmem_limit_bytes=60 * 1024 * 1024
        ),
    )(
        unet_hidden,
        control_hidden,
        steps,
        scale,
        control_time_first[0],
        control_time_second[0],
        control_proj[0].T,
        unet_time_first,
        unet_time_second,
        unet_proj.T,
        control_conv_first[0],
        control_conv_second[0],
        unet_conv_first,
        unet_conv_second,
        zero_conv[0],
    )


def solution(mesh):
    in_specs = (
        P(("branch", "dp"), "mp", None),
        P("branch", None, "dp", "mp", None),
        P(None, "dp"),
        P("branch", None, "dp"),
        P(),
        P(),
        P(None, "mp"),
        P(None, "mp", None),
        P(None, "mp", None),
        P("branch", None, None),
        P("branch", None, None),
        P("branch", None, "mp"),
        P("branch", None, "mp", None),
        P("branch", None, "mp", None),
        P("branch", "mp", None),
    )
    out_specs = P(("branch", "dp"), "mp", None)
    return jax.shard_map(shards, mesh=mesh, in_specs=in_specs, out_specs=out_specs, check_vma=False)
```

```python
import functools
import math

import jax
import jax.numpy as jnp
from jax import lax
from jax.experimental import pallas as pl
from jax.experimental.pallas import tpu as pltpu
from jax.sharding import PartitionSpec as P

TDIM = 320
GROUP = 40
PIECES = 2
PAIR_PIECES = 4
EDGE_FIRST = 2
SIDE = 16
MESH = pl.DeviceIdType.MESH


def sinusoid(steps, rows):
    half_width = TDIM // 2
    row = lax.broadcasted_iota(jnp.int32, (rows, TDIM), 0)
    spot = lax.broadcasted_iota(jnp.int32, (rows, TDIM), 1)
    place = jnp.where(spot < half_width, spot, spot - half_width).astype(jnp.float32)
    frequency = jnp.exp(-math.log(10000.0) * place / half_width)
    step = jnp.zeros((rows, TDIM), jnp.float32)
    for i, value in enumerate(steps):
        step = jnp.where(row == i, value.astype(jnp.float32), step)
    angles = step * frequency
    return jnp.where(spot < half_width, jnp.cos(angles), jnp.sin(angles))


def norm_silu(values):
    width, pixels = values.shape
    grouped = values.reshape(width // GROUP, GROUP, pixels)
    count = 1.0 / (GROUP * pixels)
    mean = jnp.sum(jnp.sum(grouped, axis=1, keepdims=True), axis=2, keepdims=True) * count
    centered = grouped - mean
    var = jnp.sum(jnp.sum(centered * centered, axis=1, keepdims=True), axis=2, keepdims=True) * count
    normed = centered * lax.rsqrt(var + 1e-05)
    return jax.nn.silu(normed).reshape(width, pixels)


def kernel(
    ways,
    unet_hidden,
    control_hidden,
    steps,
    scale,
    hbm_time_first_c,
    hbm_time_second_c,
    hbm_proj_c,
    hbm_time_first_u,
    hbm_time_second_u,
    hbm_proj_u,
    first_c,
    second_c,
    first_u,
    second_u,
    zero,
    out,
    time_first,
    time_second,
    proj,
    w1c,
    w2c,
    w1u,
    w2u,
    wz,
    gathered,
    above,
    below,
    taps,
    start,
    inner,
    sends,
    lands,
    far,
    pair_lands,
    pair_total,
    held,
    scaled,
    swap_out,
    swap_in,
    load_sem,
    ag_send,
    ag_recv,
    rs_send,
    rs_recv,
    far_recv,
    pair_send,
    pair_recv,
    z_send,
    z_recv,
    swap_send,
    swap_recv,
):
    branch = lax.axis_index("branch")
    dp = lax.axis_index("dp")
    me = lax.axis_index("mp")
    width, pixels = unet_hidden.shape[1], unet_hidden.shape[2]
    channels = ways * width
    last = ways - 1
    tile = 256
    chunks = channels // tile
    scope = jax.named_scope

    loads = [
        pltpu.make_async_copy(src, dst, load_sem.at[i])
        for i, (src, dst) in enumerate(
            (
                (hbm_time_first_c, time_first.at[0]),
                (hbm_time_second_c, time_second.at[0]),
                (hbm_proj_c, proj.at[0]),
                (hbm_time_first_u, time_first.at[1]),
                (hbm_time_second_u, time_second.at[1]),
                (hbm_proj_u, proj.at[1]),
                (first_c, w1c),
                (second_c, w2c),
                (first_u, w1u),
                (second_u, w2u),
                (zero, wz.at[pl.ds(pl.multiple_of(lax.rem(me, 2) * width, width), width)]),
            )
        )
    ]
    for i in (0, 1, 2, 6):
        loads[i].start()

    barrier = pltpu.get_barrier_semaphore()

    def greet(inside, coord):
        @pl.when(inside)
        def _():
            pl.semaphore_signal(barrier, inc=1, device_id=coord, device_id_type=MESH)

    greet(me < last, (branch, dp, me + 1))
    greet(me > 0, (branch, dp, me - 1))
    pl.semaphore_signal(barrier, inc=1, device_id=(1 - branch, dp, me), device_id_type=MESH)

    planes = lax.axis_size("dp")
    for place in range(planes):

        @pl.when(dp != place)
        def _():
            pl.semaphore_signal(barrier, inc=1, device_id=(branch, place, me), device_id_type=MESH)

    def wait_barrier():
        rim = (me == 0) | (me == last)

        @pl.when(rim)
        def _():
            pl.semaphore_wait(barrier, 1 + planes)

        @pl.when(jnp.logical_not(rim))
        def _():
            pl.semaphore_wait(barrier, 2 + planes)

    def rows_of(slot, piece=None):
        if piece is None:
            return pl.ds(pl.multiple_of(slot * width, width), width)
        size = width // PIECES
        return pl.ds(pl.multiple_of(slot * width + piece * size, size), size)

    def strip(piece):
        return pl.ds(piece * (width // PIECES), width // PIECES)

    middle = ways // 2
    low, high = me < middle, me >= middle

    def ag_copy(unit, side, hop, slot, piece):
        return pltpu.make_async_remote_copy(
            src_ref=gathered.at[unit, rows_of(slot, piece)],
            dst_ref=gathered.at[unit, rows_of(slot, piece)],
            send_sem=ag_send.at[unit, side, hop, piece],
            recv_sem=ag_recv.at[unit, side, hop, piece],
            device_id=(branch, dp, me + 1 - 2 * side),
            device_id_type=MESH,
        )


    def forward(unit, hop, sides):
        for piece in range(PIECES):
            for side, half in ((0, low), (1, high), (0, high), (1, low)):
                if half is (high if side == 0 else low) and sides is inward:
                    continue
                if half is (low if side == 0 else high) and sides is outward:
                    continue
                from_slot = me - hop if side == 0 else me + hop
                here = (from_slot >= 0) & (from_slot <= last)
                onward = here & ((me < last) if side == 0 else (me > 0)) & half & sides[side]

                @pl.when(onward)
                def _():
                    if hop > 0:
                        ag_copy(unit, side, hop - 1, from_slot, piece).wait_recv()
                    ag_copy(unit, side, hop, from_slot, piece).start()

    low, high = me < middle, me >= middle

    def ag_copy(unit, side, hop, slot, piece):
        return pltpu.make_async_remote_copy(
            src_ref=gathered.at[unit, rows_of(slot, piece)],
            dst_ref=gathered.at[unit, rows_of(slot, piece)],
            send_sem=ag_send.at[unit, side, hop, piece],
            recv_sem=ag_recv.at[unit, side, hop, piece],
            device_id=(branch, dp, me + 1 - 2 * side),
            device_id_type=MESH,
        )


    def forward(unit, hop, sides):
        for piece in range(PIECES):
            for side in range(2):
                from_slot = me - hop if side == 0 else me + hop
                here = (from_slot >= 0) & (from_slot <= last)
                onward = here & ((me < last) if side == 0 else (me > 0)) & sides[side]

                @pl.when(onward)
                def _():
                    if hop > 0:
                        ag_copy(unit, side, hop - 1, from_slot, piece).wait_recv()
                    ag_copy(unit, side, hop, from_slot, piece).start()

    edge = (me == 0) | (me == last)
    centre = jnp.logical_not(edge)
    inner_low, inner_high = low & jnp.logical_not(edge), high & jnp.logical_not(edge)
    both, inward, outward = (True, True), (low, high), (high, low)
    early, late = branch == 1, branch == 0
    outward_early, outward_late = (high & early, low & early), (high & late, low & late)

    def ag_begin(unit, sides=both):
        forward(unit, 0, sides)

    def ag_inward(unit):
        for hop in range(1, last):
            forward(unit, hop, inward)

    def ag_outward(unit, hop):
        forward(unit, hop, outward)

    def ag_arrive(unit, passed):
        for hop in passed:
            for side in range(2):
                from_slot = me - hop if side == 0 else me + hop
                here = (from_slot >= 0) & (from_slot <= last)
                if hop < last:
                    here = here & ((me == last) if side == 0 else (me == 0))

                @pl.when(here)
                def _():
                    for piece in range(PIECES):
                        ag_copy(unit, side, hop - 1, from_slot, piece).wait_recv()

    def ag_drain(unit):
        for hop in range(last):
            for side in range(2):
                from_slot = me - hop if side == 0 else me + hop
                here = (from_slot >= 0) & (from_slot <= last)
                onward = here & ((me < last) if side == 0 else (me > 0))

                @pl.when(onward)
                def _():
                    for piece in range(PIECES):
                        ag_copy(unit, side, hop, from_slot, piece).wait_send()

    def rs_copy(side, dest, piece):
        return pltpu.make_async_remote_copy(
            src_ref=sends.at[2, rows_of(dest, piece)],
            dst_ref=lands.at[side, dest, strip(piece)],
            send_sem=rs_send.at[dest, piece],
            recv_sem=rs_recv.at[side, dest, piece],
            device_id=(branch, dp, me + 1 - 2 * side),
            device_id_type=MESH,
        )

    def far_copy(dest, piece):
        return pltpu.make_async_remote_copy(
            src_ref=sends.at[2, rows_of(dest, piece)],
            dst_ref=far.at[strip(piece)],
            send_sem=rs_send.at[dest, piece],
            recv_sem=far_recv.at[piece],
            device_id=(branch, dp, dest),
            device_id_type=MESH,
        )

    def fold_begin(group):
        ready = EDGE_FIRST * tile // width
        for rank in range(ready) if group == 0 else range(ready, last):
            for side, end in ((0, 0), (1, last)):
                dest = last - rank if side == 0 else rank

                @pl.when(me == end)
                def _():
                    for piece in range(PIECES):
                        rs_copy(side, dest, piece).start()

        if group == 0:
            return
        for side in range(2):
            rim = middle - side
            for dest in range(rim + 1, ways) if side == 0 else range(rim):

                @pl.when((me == rim) & centre)
                def _():
                    for piece in range(PIECES):
                        rs_copy(side, dest, piece).start()

    def fold_slots():
        for rank, piece, side in [
            (r, p, d) for r in range(last - 1) for p in range(PIECES) for d in range(2)
        ]:
            dest = last - rank if side == 0 else rank
            place = me if side == 0 else last - me
            rim = (place == middle - 1) & (rank < middle)
            onward = (place >= 1) & (place != middle) & (place < last - rank)

            @pl.when(onward)
            def _():
                rs_copy(side, dest, piece).wait_recv()
                added = sends[2, rows_of(dest, piece), :].astype(jnp.float32) + lands[
                    side, dest, strip(piece), :
                ].astype(jnp.float32)
                sends[2, rows_of(dest, piece), :] = added.astype(jnp.bfloat16)

            @pl.when(onward & rim)
            def _():
                far_copy(dest, piece).start()

            @pl.when(onward & jnp.logical_not(rim))
            def _():
                rs_copy(side, dest, piece).start()

    def fold_drain():
        for dest in range(ways):

            @pl.when(me != dest)
            def _():
                for piece in range(PIECES):
                    rs_copy(0, dest, piece).wait_send()

    double = 2 * width
    pairs = ways // 2
    mine = me // 2
    parity = lax.rem(me, 2)
    inwards = jnp.where(low, me + 1, me - 1)
    side_near = jnp.where(low, 0, 1)
    side_far = jnp.where(low, 1, 0)
    part = double // PAIR_PIECES

    def pair_copy(unit, side, pair, piece):
        return pltpu.make_async_remote_copy(
            src_ref=sends.at[unit, pl.ds(pair * double + piece * part, part)],
            dst_ref=pair_lands.at[unit, side, pair, pl.ds(piece * part, part)],
            send_sem=pair_send.at[unit, pair, piece],
            recv_sem=pair_recv.at[unit, side, pair, piece],
            device_id=(branch, dp, me + 1 - 2 * side),
            device_id_type=MESH,
        )

    def pair_order(side):
        return range(pairs - 1, -1, -1) if side == 0 else range(pairs)

    def pair_begin(unit):
        for side, end in ((0, 0), (1, last)):

            @pl.when(me == end)
            def _():
                for pair in pair_order(side):
                    if pair != end // 2:
                        for piece in range(PAIR_PIECES):
                            pair_copy(unit, side, pair, piece).start()

    def pair_slot(unit):
        for side in range(2):
            for pair in pair_order(side):
                beyond = (pair > mine) if side == 0 else (pair < mine)

                @pl.when(centre & beyond)
                def _():
                    for piece in range(PAIR_PIECES):
                        pair_copy(unit, side, pair, piece).wait_recv()
                        rows = pl.ds(pair * double + piece * part, part)
                        added = sends[unit, rows, :].astype(jnp.float32) + pair_lands[
                            unit, side, pair, pl.ds(piece * part, part), :
                        ].astype(jnp.float32)
                        sends[unit, rows, :] = added.astype(jnp.bfloat16)
                        pair_copy(unit, side, pair, piece).start()

    def pair_drain(unit):
        for pair in range(pairs):
            for side, beyond in ((0, pair > mine), (1, pair < mine)):

                @pl.when(beyond)
                def _():
                    for piece in range(PAIR_PIECES):
                        pair_copy(unit, side, pair, piece).wait_send()

    shares = math.gcd(width // 8, planes)
    share = width // shares
    sharing = dp < shares
    mate = me + 1 - 2 * parity

    def share_rows(holder, place):
        row = lax.rem(holder, 2) * width + place * share
        return pl.ds(pl.multiple_of(row, share), share)

    def cross_copy():
        return pltpu.make_async_remote_copy(
            src_ref=zero.at[pl.ds(pl.multiple_of(dp * share, share), share)],
            dst_ref=wz.at[share_rows(me, dp)],
            send_sem=z_send.at[dp],
            recv_sem=z_recv.at[dp],
            device_id=(branch, dp, mate),
            device_id_type=MESH,
        )

    def cross_begin(chosen):
        @pl.when(chosen & sharing)
        def _():
            cross_copy().start()

    def plane_copy(source, target):
        return pltpu.make_async_remote_copy(
            src_ref=wz.at[share_rows(mate, source)],
            dst_ref=wz.at[share_rows(mate, source)],
            send_sem=z_send.at[target],
            recv_sem=z_recv.at[source],
            device_id=(branch, target, me),
            device_id_type=MESH,
        )

    def plane_begin():
        @pl.when(sharing)
        def _():
            cross_copy().wait_recv()

        for place in range(planes):

            @pl.when(sharing & (dp != place))
            def _():
                plane_copy(dp, place).start()

    def plane_arrive():
        loads[10].wait()
        for place in range(shares):

            @pl.when(dp != place)
            def _():
                plane_copy(place, place).wait_recv()

    def plane_drain():
        @pl.when(sharing)
        def _():
            cross_copy().wait_send()

        for place in range(planes):

            @pl.when(sharing & (dp != place))
            def _():
                plane_copy(dp, place).wait_send()

    def own_hidden(unit):
        if unit == 2:
            return unet_hidden[0]
        image = 1 - branch if unit == 0 else branch
        return control_hidden[0, image, 0]

    def prepare(unit):
        gathered[unit, rows_of(me), :] = norm_silu(own_hidden(unit).astype(jnp.float32)).astype(
            jnp.bfloat16
        )

    def embed(block, waves):
        for load in loads[3 * block : 3 * block + 3]:
            load.wait()
        act = waves
        for weight in (time_first, time_second):
            act = jax.nn.silu(
                jnp.dot(act, weight[block], preferred_element_type=jnp.float32)
            ).astype(jnp.bfloat16)
        start[block] = lax.dot_general(
            proj[block], act, (((1,), (1,)), ((), ())), preferred_element_type=jnp.float32
        )

    def column_kept(shape, axis, dx):
        spot = lax.rem(lax.broadcasted_iota(jnp.int32, shape, axis), SIDE) + dx
        return (spot >= 0) & (spot < SIDE)

    def shift_rows(unit, rows):
        spot = lax.broadcasted_iota(jnp.int32, (1, pixels), 1)
        whole = gathered[unit, rows, :].astype(jnp.float32)
        down = pltpu.roll(whole, SIDE, 1)
        above[rows, :] = jnp.where(spot >= SIDE, down, 0.0).astype(jnp.bfloat16)
        up = pltpu.roll(whole, pixels - SIDE, 1)
        below[rows, :] = jnp.where(spot < pixels - SIDE, up, 0.0).astype(jnp.bfloat16)

    def first_conv(unit, weight, half=None):
        if half is None:
            rows = slice(0, channels)
        else:
            rows = pl.ds(pl.multiple_of(half * (channels // 2), channels // 2), channels // 2)
        shift_rows(unit, rows)

        def side_term(dx):
            term = None
            sources = (above[rows, :], gathered[unit, rows, :], below[rows, :])
            for line, source in enumerate(sources):
                product = jnp.dot(
                    weight[3 * line + dx + 1, :, rows],
                    source,
                    preferred_element_type=jnp.float32,
                )
                term = product if term is None else term + product
            return term

        if half is side_far:
            inner[...] += side_term(0)
        else:
            other = branch == 1 if unit == 0 else branch == 0
            columns = start[unit // 2]
            inner[...] = side_term(0) + jnp.where(other, columns[:, :1], columns[:, 1:2])
        for dx in (-1, 1):
            moved = pltpu.roll(side_term(dx), (pixels - dx) % pixels, 1)
            inner[...] += jnp.where(column_kept((1, pixels), 1, dx), moved, 0.0)

    def fill_taps():
        flipped = norm_silu(inner[...]).T
        operands = []
        for dx in (-1, 0, 1):
            moved = flipped if dx == 0 else pltpu.roll(flipped, (pixels - dx) % pixels, 0)
            operands.append(jnp.where(column_kept((pixels, 1), 0, dx), moved, 0.0))
        taps[SIDE : SIDE + pixels, :] = jnp.concatenate(operands, axis=1).astype(jnp.bfloat16)


    def columns_of(chunk):
        return slice(chunk * tile, (chunk + 1) * tile)

    def second_chunk(weight, chunk):
        total = None
        for line in range(3):
            product = jnp.dot(
                taps[SIDE * line : SIDE * line + pixels, :],
                weight[3 * line : 3 * line + 3, :, columns_of(chunk)].reshape(3 * width, tile),
                preferred_element_type=jnp.float32,
            )
            total = product if total is None else total + product
        return total

    def residual_chunk(chunk):
        return jnp.dot(
            scaled[...], wz[:, columns_of(chunk)], preferred_element_type=jnp.float32
        )

    def swapped(chunk):
        return swap_in[:, columns_of(chunk)].astype(jnp.float32)

    def edge_residual():
        first_residual()
        scale_copy(1)
        for chunk in range(chunks):
            held[columns_of(chunk), :] = residual_chunk(chunk).T

    def second_conv(unit, weight):
        for chunk in range(chunks):
            total = second_chunk(weight, chunk)
            sends[unit, columns_of(chunk), :] = total.T.astype(jnp.bfloat16)
        pair_begin(unit)

    def edge_conv(order, first):
        for chunk in order[:first]:
            at = columns_of(chunk)
            total = second_chunk(w2u, chunk) + swapped(chunk)
            sends[2, at, :] = (held[at, :] + total.T).astype(jnp.bfloat16)

    def edge_last():
        for half, order in ((low, range(chunks - 1, -1, -1)), (high, range(chunks))):

            @pl.when(half)
            def _():
                edge_conv(order, EDGE_FIRST)
                if EDGE_FIRST < chunks:
                    fold_begin(0)
                    edge_conv(order[EDGE_FIRST:], chunks)

        if EDGE_FIRST == chunks:
            fold_begin(0)
        fold_begin(1)

    def centre_conv():
        for chunk in range(chunks):
            held[columns_of(chunk), :] = second_chunk(w2u, chunk).T

    def centre_last():
        for chunk in range(chunks):
            at = columns_of(chunk)
            total = residual_chunk(chunk) + swapped(chunk)
            sends[2, at, :] = (held[at, :] + total.T).astype(jnp.bfloat16)
        fold_begin(1)

    def collect():
        inner[...] = own_hidden(2).astype(jnp.float32) + sends[2, rows_of(me), :].astype(
            jnp.float32
        )
        left, right = (me > 0) & (me != middle), (me < last) & (me != middle - 1)
        for side, inside in ((0, left), (1, right)):

            @pl.when(inside)
            def _():
                for piece in range(PIECES):
                    rs_copy(side, me, piece).wait_recv()
                inner[...] += lands[side, me].astype(jnp.float32)

        for piece in range(PIECES):
            far_copy(inwards, piece).wait_recv()
        return inner[...] + far[...].astype(jnp.float32)

    def scale_copy(unit):
        image = 1 - branch if unit == 0 else branch
        factor = scale[0, image].astype(jnp.float32) * 0.125
        pair_total[...] = sends[
            unit, pl.ds(pl.multiple_of(mine * double, double), double), :
        ].astype(jnp.float32)
        own = pl.ds(pl.multiple_of(parity * width, width), width)
        pair_total[own, :] += own_hidden(unit).astype(jnp.float32)
        for pair in range(pairs):
            for side in range(2):

                @pl.when(centre & (mine == pair) & (parity == side))
                def _():
                    for piece in range(PAIR_PIECES):
                        pair_copy(unit, side, pair, piece).wait_recv()
                    pair_total[...] += pair_lands[unit, side, pair].astype(jnp.float32)

        scaled[...] = (pair_total[...] * factor).T.astype(jnp.bfloat16)

    swap = pltpu.make_async_remote_copy(
        src_ref=swap_out,
        dst_ref=swap_in,
        send_sem=swap_send,
        recv_sem=swap_recv,
        device_id=(1 - branch, dp, me),
        device_id_type=MESH,
    )

    def first_residual():
        scale_copy(0)
        swap_out[...] = jnp.dot(scaled[...], wz[...], preferred_element_type=jnp.float32).astype(
            jnp.bfloat16
        )
        swap.start()

    taps[0:SIDE, :] = jnp.zeros((SIDE, 3 * width), jnp.bfloat16)
    taps[SIDE + pixels :, :] = jnp.zeros((SIDE, 3 * width), jnp.bfloat16)

    hops = range(1, last)
    with scope("prep"):
        for unit in range(3):
            prepare(unit)
        waves = sinusoid([steps[0, i] for i in range(steps.shape[1])], 16).astype(jnp.bfloat16)
    with scope("barrier"):
        wait_barrier()
    with scope("ag0"):
        ag_begin(0)
        cross_begin(centre)
        for unit in (1, 2):
            ag_begin(unit, (me == 0, me == last))
        cross_begin(edge)
    with scope("embed0"):
        embed(0, waves)
        for i in (7, 3, 4, 5, 10):
            loads[i].start()
    for hop in hops:
        with scope(f"ag0_hop{hop}"):
            forward(0, hop, both)
            if hop == 1:
                ag_begin(1, (inner_low, inner_high))
    with scope("ag1"):
        ag_begin(1, outward)
        ag_inward(1)
    with scope("embed1"):
        embed(1, waves)
    with scope("ag0_wait"):
        ag_arrive(0, range(1, ways))
    with scope("w1c_wait"):
        loads[6].wait()
    with scope("conv1_0"):
        first_conv(0, w1c)
    with scope("ag2_in"):
        ag_begin(2, (inner_low, inner_high))
        ag_inward(2)
    with scope("ag1_out1"):
        ag_outward(1, 1)
        for i in (8, 9):
            loads[i].start()
    with scope("w2c_wait"):
        loads[7].wait()
    with scope("fill0"):
        fill_taps()
    with scope("conv2_0"):
        second_conv(0, w2c)
    for hop in hops[1:]:
        with scope(f"ag1_out{hop}"):
            ag_outward(1, hop)
    with scope("ag2"):
        ag_begin(2, outward_early)
    with scope("plane"):
        plane_begin()
    with scope("ag1_wait"):
        ag_arrive(1, range(1, ways))
    with scope("conv1_1"):
        first_conv(1, w1c)
    with scope("ag2_out1"):
        forward(2, 1, outward_early)
    with scope("fill1"):
        fill_taps()
    for hop in hops[1:]:
        with scope(f"ag2_out{hop}"):
            forward(2, hop, outward_early)
    with scope("conv2_1"):
        second_conv(1, w2c)
    with scope("rs0_slot"):
        pair_slot(0)
    with scope("ag2_late"):
        ag_begin(2, outward_late)
        for hop in hops:
            forward(2, hop, outward_late)
    with scope("plane_wait"):
        plane_arrive()
    with scope("res0e"):
        pl.when(edge)(edge_residual)
    with scope("ag2_wait"):
        ag_arrive(2, range(1, middle))
        loads[8].wait()
    with scope("conv1_2n"):
        first_conv(2, w1u, side_near)
    with scope("ag2_wait2"):
        ag_arrive(2, range(middle, ways))
        loads[9].wait()
    with scope("conv1_2f"):
        first_conv(2, w1u, side_far)
    with scope("res0c"):
        pl.when(centre)(first_residual)
    with scope("fill2"):
        fill_taps()

    @pl.when(edge)
    def _():
        with scope("swap_e"):
            swap.wait_recv()
        with scope("conv2_2e"):
            edge_last()

    @pl.when(centre)
    def _():
        with scope("conv2_2c"):
            centre_conv()
        with scope("rs1_slot"):
            pair_slot(1)
        with scope("res1c"):
            scale_copy(1)
        with scope("swap_c"):
            swap.wait_recv()
        with scope("add_c"):
            centre_last()

    with scope("rs2_slots"):
        fold_slots()
    with scope("collect2"):
        out[0] = collect().astype(jnp.bfloat16)
    with scope("drain"):
        swap.wait_send()
        plane_drain()
        for unit in range(3):
            ag_drain(unit)
        for unit in range(2):
            pair_drain(unit)
        fold_drain()


def shards(
    unet_hidden,
    control_hidden,
    timesteps,
    control_scales,
    unet_time_first,
    unet_time_second,
    unet_proj,
    unet_conv_first,
    unet_conv_second,
    control_time_first,
    control_time_second,
    control_proj,
    control_conv_first,
    control_conv_second,
    zero_conv,
):
    ways, planes = lax.axis_size("mp"), lax.axis_size("dp")
    width, pixels = unet_hidden.shape[1], unet_hidden.shape[2]
    channels = ways * width
    halves = timesteps.shape[0]
    steps = timesteps.reshape(1, halves)
    scale = control_scales.reshape(1, halves)
    vmem = pl.BlockSpec(memory_space=pltpu.VMEM)
    smem = pl.BlockSpec(memory_space=pltpu.SMEM)
    hbm = pl.BlockSpec(memory_space=pl.ANY)
    taps = unet_conv_first.shape[0]
    bf16, f32 = jnp.bfloat16, jnp.float32
    conv_shape = (taps, width, channels)
    return pl.pallas_call(
        functools.partial(kernel, ways),
        out_shape=pltpu.VMEM((1, width, pixels), bf16),
        in_specs=[vmem] * 2 + [smem] * 2 + [hbm] * 11,
        out_specs=vmem,
        scratch_shapes=[
            pltpu.VMEM((2,) + unet_time_first.shape, bf16),
            pltpu.VMEM((2,) + unet_time_second.shape, bf16),
            pltpu.VMEM((2,) + unet_proj.shape[::-1], bf16),
            pltpu.VMEM(conv_shape, bf16),
            pltpu.VMEM(conv_shape, bf16),
            pltpu.VMEM(conv_shape, bf16),
            pltpu.VMEM(conv_shape, bf16),
            pltpu.VMEM((2 * width, channels), bf16),
            pltpu.VMEM((3, channels, pixels), bf16),
            pltpu.VMEM((channels, pixels), bf16),
            pltpu.VMEM((channels, pixels), bf16),
            pltpu.VMEM((pixels + 2 * SIDE, 3 * width), bf16),
            pltpu.VMEM((2, width, 16), f32),
            pltpu.VMEM((width, pixels), f32),
            pltpu.VMEM((3, channels, pixels), bf16),
            pltpu.VMEM((2, ways, width, pixels), bf16),
            pltpu.VMEM((width, pixels), bf16),
            pltpu.VMEM((2, 2, ways // 2, 2 * width, pixels), bf16),
            pltpu.VMEM((2 * width, pixels), f32),
            pltpu.VMEM((channels, pixels), f32),
            pltpu.VMEM((pixels, 2 * width), bf16),
            pltpu.VMEM((pixels, channels), bf16),
            pltpu.VMEM((pixels, channels), bf16),
            pltpu.SemaphoreType.DMA((11,)),
            pltpu.SemaphoreType.DMA((3, 2, ways - 1, PIECES)),
            pltpu.SemaphoreType.DMA((3, 2, ways - 1, PIECES)),
            pltpu.SemaphoreType.DMA((ways, PIECES)),
            pltpu.SemaphoreType.DMA((2, ways, PIECES)),
            pltpu.SemaphoreType.DMA((PIECES,)),
            pltpu.SemaphoreType.DMA((2, ways // 2, PAIR_PIECES)),
            pltpu.SemaphoreType.DMA((2, 2, ways // 2, PAIR_PIECES)),
            pltpu.SemaphoreType.DMA((planes,)),
            pltpu.SemaphoreType.DMA((planes,)),
            pltpu.SemaphoreType.DMA,
            pltpu.SemaphoreType.DMA,
        ],
        compiler_params=pltpu.CompilerParams(
            collective_id=0, has_side_effects=True, vmem_limit_bytes=60 * 1024 * 1024
        ),
    )(
        unet_hidden,
        control_hidden,
        steps,
        scale,
        control_time_first[0],
        control_time_second[0],
        control_proj[0].T,
        unet_time_first,
        unet_time_second,
        unet_proj.T,
        control_conv_first[0],
        control_conv_second[0],
        unet_conv_first,
        unet_conv_second,
        zero_conv[0],
    )


def solution(mesh):
    in_specs = (
        P(("branch", "dp"), "mp", None),
        P("branch", None, "dp", "mp", None),
        P(None, "dp"),
        P("branch", None, "dp"),
        P(),
        P(),
        P(None, "mp"),
        P(None, "mp", None),
        P(None, "mp", None),
        P("branch", None, None),
        P("branch", None, None),
        P("branch", None, "mp"),
        P("branch", None, "mp", None),
        P("branch", None, "mp", None),
        P("branch", "mp", None),
    )
    out_specs = P(("branch", "dp"), "mp", None)
    return jax.shard_map(shards, mesh=mesh, in_specs=in_specs, out_specs=out_specs, check_vma=False)
```
